512 devices in a mesh: gx: 16 (over y, x), gy: 32 (over z, core).
Axes of the slice: x: 4, y: 4, z: 16, core: 2. Of those that a mesh axis runs over, the one named last changes fastest.
Arguments:
- posterior: bfloat16 [131072, 1000], P(('gx', 'gy')), may hold values from -6 to 6
- class_affinity: bfloat16 [131072, 1000], P(('gx', 'gy')), may hold values from 0.049804688 to 20
- band_tiles: bfloat16 [1024, 4, 128, 128], P(('gx', 'gy')), may hold values from 9.9658966e-05 to 1
- band_offset: int32 [1024, 4], P(('gx', 'gy')), may hold values from -1 to 1
- band_count: int32 [1024], P(('gx', 'gy')), may hold values from 1 to 4
- far_tiles: bfloat16 [512, 16, 128, 128], P(('gx', 'gy')), may hold values from 9.9658966e-05 to 1
- far_row: int32 [512, 16], P(('gx', 'gy')), may hold values from 0 to 1
- far_block: int32 [512, 16], P(('gx', 'gy')), may hold values from 0 to 1
Outputs:
- propagated: bfloat16 [131072, 1000], P(('gx', 'gy'))
The draws below stay inside these ranges and needn't reach their ends.
Inputs may be any that keep to these rules, and one draw needn't show every extreme that they name: Near tiles of a slot index at or above band_count of their row block are not part of the graph.
All inputs are finite; a program needn't handle non-finite values.
Results may differ from the reference program's by a relative error of at most 0.002.
Values may be sent and summed in bfloat16 or wider, within the bound.
No kernel may reach another device: no remote copies, remote signals or barrier semaphores. Data moves between devices by JAX's collectives and lax.ppermute only.
A program may use at most 64 MiB of HBM per device.

```python
import math
import jax
import jax.numpy as jnp
from jax import lax

CLASSES = 1000
TILE_SIZE = 128
BLOCKS_DEV = 2
SLOTS = 4
BAND_REACH = 1
SWEEPS = 2
ALL_BLOCKS = 1024
ALL_NODES = 131072
N_GX = 16
N_GY = 32
DEVICES = 512


def touch_ends(result, own_key, low, top_value):
    longest = result.shape.index(max(result.shape))
    spots = []
    for shift in (0, 1):
        where = [jax.random.randint(jax.random.fold_in(own_key, axis), (), 0, length) for axis, length in enumerate(result.shape)]
        where[longest] = (where[longest] + shift) % result.shape[longest]
        spots.append(tuple(where))
    return result.at[spots[0]].set(low).at[spots[1]].set(top_value)


def block_levels(stream_key, shape, shards, low, largest):
    def one(axis_at, blocks):
        draws = jax.random.uniform(jax.random.fold_in(jax.random.fold_in(stream_key, 6), axis_at), (blocks,), jnp.float32, low / len(shards), largest / len(shards))
        return jnp.repeat(jnp.exp(draws), shape[axis_at] // blocks).reshape((-1,) + (1,) * (len(shape) - axis_at - 1))

    factor_of = one(*shards[0])
    for cut in shards[1:]:
        factor_of = factor_of * one(*cut)
    return factor_of


def scatter_about(own_key, dims, deviation, most, cuts=(), kind=jnp.bfloat16):
    drawn = jax.random.normal(own_key, dims, jnp.float32) * deviation
    if len(cuts) > 0:
        drawn = block_levels(own_key, dims, cuts, -0.22, 0.18) * drawn
    return jnp.clip(drawn, min=-most, max=most).astype(kind)


def setup_inputs(seed: int = 0) -> dict:
    splits = jax.random.split(jax.random.key(seed), 9)
    posterior = scatter_about(splits[0], (ALL_NODES, CLASSES), 1.0, 6.0, ((0, 512),))
    class_affinity = jnp.clip(jnp.exp(math.log(20.0) - 5.9953784 * jax.random.uniform(splits[1], (ALL_NODES, CLASSES), jnp.float32) ** block_levels(splits[1], (ALL_NODES, CLASSES), ((0, 512),), -0.2, 0.2)), 0.049804688, 20.0).astype(jnp.bfloat16)
    band_tiles = jnp.clip(jnp.exp(math.log(1.0) - 9.213757 * jax.random.uniform(splits[2], (ALL_BLOCKS, SLOTS, TILE_SIZE, TILE_SIZE), jnp.float32) ** block_levels(splits[2], (ALL_BLOCKS, SLOTS, TILE_SIZE, TILE_SIZE), ((0, 512),), -0.2, 0.2)), 9.965896606445312e-05, 1.0).astype(jnp.bfloat16)
    band_offset = touch_ends(jax.random.randint(splits[3], (ALL_BLOCKS, SLOTS), 0 - BAND_REACH, BAND_REACH + 1), jax.random.fold_in(splits[3], 1), 0 - BAND_REACH, BAND_REACH).astype(jnp.int32)
    band_count = touch_ends(jax.random.randint(splits[4], (ALL_BLOCKS,), 1, SLOTS + 1), jax.random.fold_in(splits[4], 1), 1, SLOTS).astype(jnp.int32)
    far_tiles = jnp.clip(jnp.exp(math.log(1.0) - 9.213757 * jax.random.uniform(splits[5], (DEVICES, N_GX, TILE_SIZE, TILE_SIZE), jnp.float32) ** block_levels(splits[5], (DEVICES, N_GX, TILE_SIZE, TILE_SIZE), ((0, 512),), -0.2, 0.2)), 9.965896606445312e-05, 1.0).astype(jnp.bfloat16)
    far_row = touch_ends(jax.random.randint(splits[6], (DEVICES, N_GX), 0, BLOCKS_DEV), jax.random.fold_in(splits[6], 1), 0, BLOCKS_DEV - 1).astype(jnp.int32)
    far_block = touch_ends(jax.random.randint(splits[7], (DEVICES, N_GX), 0, BLOCKS_DEV), jax.random.fold_in(splits[7], 1), 0, BLOCKS_DEV - 1).astype(jnp.int32)
    return dict(posterior=posterior, class_affinity=class_affinity, band_tiles=band_tiles, band_offset=band_offset, band_count=band_count, far_tiles=far_tiles, far_row=far_row, far_block=far_block)


propagation_weight = 0.9
epsilon = 1e-06

def normalize(mixed_rows):
    row_scale = lax.rsqrt(lax.optimization_barrier(jnp.mean(mixed_rows * mixed_rows, axis=-1, keepdims=True)) + epsilon)
    return (mixed_rows * row_scale).astype(jnp.bfloat16)

def reference(posterior, class_affinity, band_tiles, band_offset, band_count, far_tiles, far_row, far_block):
    class_count = posterior.shape[1]
    device_count = N_GX * N_GY
    group_blocks = BLOCKS_DEV * N_GY
    slot_ids = jnp.arange(SLOTS, dtype=jnp.int32)
    peer_ids = jnp.arange(N_GX, dtype=jnp.int32)
    block_ids = jnp.arange(BLOCKS_DEV, dtype=jnp.int32)
    current = posterior
    for sweep in range(SWEEPS):
        blocks_all = current.reshape(device_count * BLOCKS_DEV, TILE_SIZE, class_count)

        def one_device(device):
            device = device.astype(jnp.int32)
            outer_index = device // N_GY
            inner_index = device % N_GY
            first_block = device * BLOCKS_DEV
            rows_here = first_block + block_ids
            tile_block = lax.dynamic_slice_in_dim(band_tiles, first_block, BLOCKS_DEV, 0)
            offsets = lax.dynamic_slice_in_dim(band_offset, first_block, BLOCKS_DEV, 0)
            counts = lax.dynamic_slice_in_dim(band_count, first_block, BLOCKS_DEV, 0)
            group_base = outer_index * group_blocks
            columns = (group_base + (rows_here[:, None] - group_base + offsets) % group_blocks).astype(jnp.int32)
            live_mask = (slot_ids[None, :] < counts[:, None]).astype(jnp.float32)
            sources = blocks_all[columns]
            band_sum = jnp.einsum('bsij,bsjc->bic', tile_block.astype(jnp.float32) * live_mask[:, :, None, None], sources.astype(jnp.float32))
            far_block_tiles = far_tiles[device]
            far_rows = far_row[device]
            far_source = far_block[device]
            far_columns = ((peer_ids * N_GY + inner_index) * BLOCKS_DEV + far_source).astype(jnp.int32)
            far_sources = blocks_all[far_columns]
            far_parts = jnp.einsum('qij,qjc->qic', far_block_tiles.astype(jnp.float32), far_sources.astype(jnp.float32))
            owner_table = (far_rows[None, :] == block_ids[:, None]).astype(jnp.float32)
            far_sum = jnp.einsum('bq,qic->bic', owner_table, far_parts)
            combined = (band_sum + far_sum).reshape(BLOCKS_DEV * TILE_SIZE, class_count)
            affinity_rows = lax.dynamic_slice_in_dim(class_affinity, first_block * TILE_SIZE, BLOCKS_DEV * TILE_SIZE, 0)
            mixed_rows = propagation_weight * combined + affinity_rows.astype(jnp.float32)
            return normalize(mixed_rows)
        current = lax.map(one_device, jnp.arange(device_count, dtype=jnp.int32)).reshape(device_count * BLOCKS_DEV * TILE_SIZE, class_count)
    return current
```

```python
import jax
import jax.numpy as jnp
import numpy as np
from jax import lax
from jax.experimental import pallas as pl
from jax.experimental.pallas import tpu as pltpu
from jax.sharding import Mesh, PartitionSpec as P

SWEEPS = 2
SIDE = 4
PEERS = 4
CODE_ROWS = 16
CODE_BITS = 13
CHUNK = 112
POWER_ROWS = 8

propagation_weight = 0.9
epsilon = 1e-06

VMEM = pl.BlockSpec(memory_space=pltpu.VMEM)
SMEM = pl.BlockSpec(memory_space=pltpu.SMEM)
MIB = 1024 * 1024


def squares(shift):
    return [
        [((2 * i + k - shift) % SIDE) * SIDE + (2 * j + m - shift) % SIDE for k in (0, 1) for m in (0, 1)]
        for i in (0, 1)
        for j in (0, 1)
    ]


def phase_squares(core, phase):
    return squares((core + phase) % 2)


def phase_groups(inner, phase):
    return [
        [chip * inner + pos for chip in square]
        for pos in range(inner)
        for square in phase_squares(pos % 2, phase)
    ]


def tile_order():
    order = np.zeros((2, SIDE * SIDE, PEERS, PEERS), np.int32)
    for core in range(2):
        first = {chip: square for square in phase_squares(core, 0) for chip in square}
        second = {chip: square for square in phase_squares(core, 1) for chip in square}
        for chip in range(SIDE * SIDE):
            for b, middle in enumerate(second[chip]):
                order[core, chip, b] = first[middle]
    return order


def pack_kernel(order_ref, row_ref, block_ref, tiles_ref, out_ref):
    size = tiles_ref.shape[-1]
    blocks = 2
    for b in range(PEERS):
        sublane = lax.broadcasted_iota(jnp.int32, (CODE_ROWS, size), 0)
        codes = jnp.zeros((CODE_ROWS, size), jnp.float32)
        for a in range(PEERS):
            q = order_ref[b, a]
            out_ref[b, a * size : (a + 1) * size, :] = tiles_ref[q]
            code = (row_ref[q] * blocks + block_ref[q]).astype(jnp.float32)
            codes = jnp.where(sublane == a, code, codes)
        out_ref[b, PEERS * size :, :] = codes.astype(jnp.bfloat16)


def pack(order, row, block, tiles):
    size = tiles.shape[-1]
    return pl.pallas_call(
        pack_kernel,
        out_shape=jax.ShapeDtypeStruct((PEERS, PEERS * size + CODE_ROWS, size), jnp.bfloat16),
        in_specs=[SMEM, SMEM, SMEM, VMEM],
        out_specs=VMEM,
        compiler_params=pltpu.CompilerParams(vmem_limit_bytes=4 * MIB),
        name="pack",
    )(order, row, block, tiles)


def times_transposed(left, right):
    return lax.dot_general(left, right, (((1,), (1,)), ((), ())), preferred_element_type=jnp.float32)


def near_kernel(offset_ref, count_ref, before_ref, own_ref, after_ref, tiles_ref, sum_ref, ext, left, right):
    blocks, slots, size, _ = tiles_ref.shape
    ext[0] = before_ref[...]
    for b in range(blocks):
        ext[b + 1] = own_ref[:, b * size : (b + 1) * size]
    ext[blocks + 1] = after_ref[...]
    for b in range(blocks):
        for s in range(slots):
            tile = tiles_ref[b, s]
            right[:, s * size : (s + 1) * size] = jnp.where(s < count_ref[b], tile, jnp.zeros_like(tile))
            left[:, s * size : (s + 1) * size] = ext[b + 1 + offset_ref[b, s]]
        sum_ref[:, b * size : (b + 1) * size] = times_transposed(left[...], right[...])


def near_sum(offset, count, before, own, after, tiles):
    blocks, slots, size, _ = tiles.shape
    classes = own.shape[0]
    return pl.pallas_call(
        near_kernel,
        out_shape=jax.ShapeDtypeStruct((classes, blocks * size), jnp.float32),
        in_specs=[SMEM, SMEM, VMEM, VMEM, VMEM, VMEM],
        out_specs=VMEM,
        scratch_shapes=[
            pltpu.VMEM((blocks + 2, classes, size), jnp.bfloat16),
            pltpu.VMEM((classes, slots * size), jnp.bfloat16),
            pltpu.VMEM((size, slots * size), jnp.bfloat16),
        ],
        cost_estimate=pl.CostEstimate(flops=3_000_000_000, bytes_accessed=3_000_000, transcendentals=0),
        compiler_params=pltpu.CompilerParams(vmem_limit_bytes=12 * MIB),
        name="near_sum",
    )(offset, count, before, own, after, tiles)


def partial_kernel(code_ref, rows_ref, tiles_ref, out_ref, left, right, acc):
    d = pl.program_id(0)
    peers, classes, width = rows_ref.shape
    size = tiles_ref.shape[-1]
    blocks = width // size
    height = out_ref.shape[1]
    for a in range(peers):
        code = code_ref[d, a]
        tile = tiles_ref[0, a * size : (a + 1) * size, :]
        for r in range(blocks):
            right[r * size : (r + 1) * size, a * size : (a + 1) * size] = jnp.where(
                code // blocks == r, tile, jnp.zeros_like(tile)
            )
        lane = pl.multiple_of((code % blocks) * size, size)
        left[:, a * size : (a + 1) * size] = rows_ref[a, :, pl.ds(lane, size)]
    acc[:classes, :] = times_transposed(left[...], right[...])
    acc[classes:, :] = jnp.zeros((height - classes, width), jnp.float32)
    peak = jnp.max(jnp.abs(acc[...]), axis=0, keepdims=True)
    power = jnp.floor(jnp.log2(jnp.maximum(peak, 1e-30)))
    scale = jnp.exp2(CODE_BITS - power)
    for at in range(0, height, CHUNK):
        scaled = jnp.round(acc[at : at + CHUNK, :] * scale)
        if at + CHUNK > classes:
            sublane = lax.broadcasted_iota(jnp.int32, scaled.shape, 0) + at
            scaled = jnp.where(sublane < classes, scaled, power)
        out_ref[0, at : at + CHUNK, :] = scaled.astype(jnp.int32).astype(jnp.int16)


def partial_sums(code, rows, tiles):
    peers, classes, width = rows.shape
    size = tiles.shape[-1]
    height = classes + POWER_ROWS
    return pl.pallas_call(
        partial_kernel,
        out_shape=jax.ShapeDtypeStruct((peers, height, width), jnp.int16),
        grid=(peers,),
        in_specs=[
            SMEM,
            pl.BlockSpec((peers, classes, width), lambda d: (0, 0, 0)),
            pl.BlockSpec((1, tiles.shape[1], size), lambda d: (d, 0, 0)),
        ],
        out_specs=pl.BlockSpec((1, height, width), lambda d: (d, 0, 0)),
        scratch_shapes=[
            pltpu.VMEM((classes, peers * size), jnp.bfloat16),
            pltpu.VMEM((width, peers * size), jnp.bfloat16),
            pltpu.VMEM((height, width), jnp.float32),
        ],
        compiler_params=pltpu.CompilerParams(vmem_limit_bytes=16 * MIB),
        name="partial_sums",
    )(code, rows, tiles)


def combine_kernel(copies, near_ref, parts_ref, affinity_ref, *refs):
    peers = parts_ref.shape[0]
    classes, width = near_ref.shape
    out_refs, mixed_ref = refs[:-1], refs[-1]
    power_at = classes - POWER_ROWS
    scales = []
    for p in range(peers):
        power = parts_ref[p, power_at:, :].astype(jnp.int32).astype(jnp.float32)[POWER_ROWS : POWER_ROWS + 1, :]
        scales.append(jnp.exp2(power - CODE_BITS))
    square = jnp.zeros((1, width), jnp.float32)
    for start in range(0, classes, CHUNK):
        at = slice(start, min(start + CHUNK, classes))
        total = near_ref[at, :]
        for p in range(peers):
            total += parts_ref[p, at, :].astype(jnp.int32).astype(jnp.float32) * scales[p]
        mixed = propagation_weight * total + affinity_ref[at, :].astype(jnp.float32)
        mixed_ref[at, :] = mixed
        square += jnp.sum(mixed * mixed, axis=0, keepdims=True)
    row_scale = lax.rsqrt(square * (1.0 / classes) + epsilon)
    for start in range(0, classes, CHUNK):
        at = slice(start, min(start + CHUNK, classes))
        result = (mixed_ref[at, :] * row_scale).astype(jnp.bfloat16)
        out_refs[0][at, :] = result
        for n in range(copies):
            out_refs[1][n, at, :] = result


def combine(near, parts, affinity, copies):
    shapes = [jax.ShapeDtypeStruct(near.shape, jnp.bfloat16)]
    if copies:
        shapes.append(jax.ShapeDtypeStruct((copies,) + near.shape, jnp.bfloat16))
    return pl.pallas_call(
        lambda *refs: combine_kernel(copies, *refs),
        out_shape=shapes,
        in_specs=[VMEM, VMEM, VMEM],
        out_specs=[VMEM] * len(shapes),
        scratch_shapes=[pltpu.VMEM(near.shape, jnp.float32)],
        compiler_params=pltpu.CompilerParams(vmem_limit_bytes=16 * MIB),
        name="combine",
    )(near, parts, affinity)


def local(inner, posterior, class_affinity, band_tiles, band_offset, band_count, far_tiles, far_row, far_block):
    size = band_tiles.shape[2]
    chips = SIDE * SIDE
    ring = [(x * inner + j, x * inner + (j + 1) % inner) for x in range(chips) for j in range(inner)]
    back = [(j, i) for i, j in ring]
    device = lax.axis_index("d")
    order = jnp.asarray(tile_order())[(device % inner) % 2, device // inner]

    def exchange(value, phase):
        return lax.all_to_all(value, "d", 0, 0, tiled=True, axis_index_groups=phase_groups(inner, phase))

    payload = exchange(
        pack(order, far_row.reshape(chips), far_block.reshape(chips), far_tiles.reshape(chips, size, size)), 1
    )
    code = payload[:, PEERS * size : PEERS * size + PEERS, 0].astype(jnp.int32)

    current = posterior.T
    affinity = class_affinity.T
    copies = jnp.broadcast_to(current[None], (PEERS,) + current.shape)
    for sweep in range(SWEEPS):
        arrived = exchange(copies, 0)
        before = lax.ppermute(current[:, -size:], "d", ring)
        after = lax.ppermute(current[:, :size], "d", back)
        near = near_sum(band_offset, band_count, before, current, after, band_tiles)
        parts = exchange(partial_sums(code, arrived, payload), 1)
        last = sweep == SWEEPS - 1
        result = combine(near, parts, affinity, 0 if last else PEERS)
        if last:
            return result[0].T
        current, copies = result


def solution(mesh):
    inner = mesh.shape["gy"]
    flat = Mesh(mesh.devices.reshape(-1), ("d",))
    spec = P("d")
    return jax.shard_map(
        lambda *args: local(inner, *args), mesh=flat, in_specs=(spec,) * 8, out_specs=spec, check_vma=False
    )
```

```python
import jax
import jax.numpy as jnp
import numpy as np
from jax import lax
from jax.experimental import pallas as pl
from jax.experimental.pallas import tpu as pltpu
from jax.sharding import Mesh, PartitionSpec as P

SWEEPS = 2
SIDE = 4
PEERS = 4
PARTNERS = (3, 1, 2)
CODE_ROWS = 16
CODE_BITS = 13
CHUNK = 112
POWER_ROWS = 8

propagation_weight = 0.9
epsilon = 1e-06

VMEM = pl.BlockSpec(memory_space=pltpu.VMEM)
SMEM = pl.BlockSpec(memory_space=pltpu.SMEM)
MIB = 1024 * 1024


def squares(shift):
    return [
        [((2 * i + k - shift) % SIDE) * SIDE + (2 * j + m - shift) % SIDE for k in (0, 1) for m in (0, 1)]
        for i in (0, 1)
        for j in (0, 1)
    ]


def partner_table(core, phase):
    table = {}
    for square in squares((core + phase) % 2):
        for place, chip in enumerate(square):
            table[chip] = [square[place ^ s] for s in range(PEERS)]
    return table


def partner_pairs(inner, phase, s):
    return [
        (chip * inner + pos, partner_table(pos % 2, phase)[chip][s] * inner + pos)
        for pos in range(inner)
        for chip in range(SIDE * SIDE)
    ]


def square_groups(inner, phase):
    return [
        [chip * inner + pos for chip in square] for pos in range(inner) for square in squares((pos + phase) % 2)
    ]


def tile_order():
    order = np.zeros((2, SIDE * SIDE, PEERS, PEERS), np.int32)
    for core in range(2):
        first = partner_table(core, 0)
        for square in squares((core + 1) % 2):
            for chip in square:
                for b, middle in enumerate(square):
                    order[core, chip, b] = first[middle]
    return order


def pack_kernel(order_ref, row_ref, block_ref, tiles_ref, out_ref):
    size = tiles_ref.shape[-1]
    blocks = 2
    for b in range(PEERS):
        sublane = lax.broadcasted_iota(jnp.int32, (CODE_ROWS, size), 0)
        codes = jnp.zeros((CODE_ROWS, size), jnp.float32)
        for a in range(PEERS):
            q = order_ref[b, a]
            out_ref[b, a * size : (a + 1) * size, :] = tiles_ref[q]
            code = (row_ref[q] * blocks + block_ref[q]).astype(jnp.float32)
            codes = jnp.where(sublane == a, code, codes)
        out_ref[b, PEERS * size :, :] = codes.astype(jnp.bfloat16)


def pack(order, row, block, tiles):
    size = tiles.shape[-1]
    return pl.pallas_call(
        pack_kernel,
        out_shape=jax.ShapeDtypeStruct((PEERS, PEERS * size + CODE_ROWS, size), jnp.bfloat16),
        in_specs=[SMEM, SMEM, SMEM, VMEM],
        out_specs=VMEM,
        compiler_params=pltpu.CompilerParams(vmem_limit_bytes=4 * MIB),
        name="pack",
    )(order, row, block, tiles)


def times_transposed(left, right):
    return lax.dot_general(left, right, (((1,), (1,)), ((), ())), preferred_element_type=jnp.float32)


def fill(code_ref, d, source_refs, tiles_ref, left, right):
    size = tiles_ref.shape[-1]
    for a, source_ref in enumerate(source_refs):
        code = code_ref[d, a]
        tile = tiles_ref[d, a * size : (a + 1) * size, :]
        for r in range(2):
            right[r * size : (r + 1) * size, a * size : (a + 1) * size] = jnp.where(
                code // 2 == r, tile, jnp.zeros_like(tile)
            )
        lane = pl.multiple_of((code % 2) * size, size)
        left[:, a * size : (a + 1) * size] = source_ref[:, pl.ds(lane, size)]


def near_kernel(core_ref, offset_ref, count_ref, own_ref, even_ref, odd_ref, tiles_ref, sum_ref, ext, left, right):
    blocks, slots, size, _ = tiles_ref.shape

    @pl.when(core_ref[0] == 0)
    def _():
        ext[0] = odd_ref[:, size:]
        ext[blocks + 1] = even_ref[:, :size]

    @pl.when(core_ref[0] != 0)
    def _():
        ext[0] = even_ref[:, size:]
        ext[blocks + 1] = odd_ref[:, :size]

    for b in range(blocks):
        ext[b + 1] = own_ref[:, b * size : (b + 1) * size]
    for b in range(blocks):
        for s in range(slots):
            tile = tiles_ref[b, s]
            right[:, s * size : (s + 1) * size] = jnp.where(s < count_ref[b], tile, jnp.zeros_like(tile))
            left[:, s * size : (s + 1) * size] = ext[b + 1 + offset_ref[b, s]]
        sum_ref[:, b * size : (b + 1) * size] = times_transposed(left[...], right[...])


def near_sum(core, offset, count, own, even, odd, tiles):
    blocks, slots, size, _ = tiles.shape
    classes, width = even.shape
    return pl.pallas_call(
        near_kernel,
        out_shape=jax.ShapeDtypeStruct((classes, width), jnp.float32),
        in_specs=[SMEM] * 3 + [VMEM] * 4,
        out_specs=VMEM,
        scratch_shapes=[
            pltpu.VMEM((blocks + 2, classes, size), jnp.bfloat16),
            pltpu.VMEM((classes, slots * size), jnp.bfloat16),
            pltpu.VMEM((size, slots * size), jnp.bfloat16),
        ],
        cost_estimate=pl.CostEstimate(flops=3_000_000_000, bytes_accessed=3_000_000, transcendentals=0),
        compiler_params=pltpu.CompilerParams(vmem_limit_bytes=12 * MIB),
        name="near_sum",
    )(core, offset, count, own, even, odd, tiles)


def partial_kernel(code_ref, *refs):
    source_refs, (tiles_ref, out_ref, left, right, acc) = refs[:PEERS], refs[PEERS:]
    classes, width = source_refs[0].shape
    height = out_ref.shape[1]
    acc[classes:, :] = jnp.zeros((height - classes, width), jnp.float32)

    for d in range(PEERS):
        fill(code_ref, d, source_refs, tiles_ref, left, right)
        acc[:classes, :] = times_transposed(left[...], right[...])
        peak = jnp.max(jnp.abs(acc[...]), axis=0, keepdims=True)
        power = jnp.floor(jnp.log2(jnp.maximum(peak, 1e-30)))
        scale = jnp.exp2(CODE_BITS - power)
        for at in range(0, height, CHUNK):
            scaled = jnp.round(acc[at : at + CHUNK, :] * scale)
            if at + CHUNK > classes:
                sublane = lax.broadcasted_iota(jnp.int32, scaled.shape, 0) + at
                scaled = jnp.where(sublane < classes, scaled, power)
            out_ref[d, at : at + CHUNK, :] = scaled.astype(jnp.int32).astype(jnp.int16)


def partial_sums(code, sources, tiles):
    classes, width = sources[0].shape
    size = tiles.shape[-1]
    height = classes + POWER_ROWS
    return pl.pallas_call(
        partial_kernel,
        out_shape=jax.ShapeDtypeStruct((PEERS, height, width), jnp.int16),
        in_specs=[SMEM] + [VMEM] * (PEERS + 1),
        out_specs=VMEM,
        scratch_shapes=[
            pltpu.VMEM((classes, PEERS * size), jnp.bfloat16),
            pltpu.VMEM((width, PEERS * size), jnp.bfloat16),
            pltpu.VMEM((height, width), jnp.float32),
        ],
        cost_estimate=pl.CostEstimate(flops=500_000_000, bytes_accessed=3_000_000, transcendentals=0),
        compiler_params=pltpu.CompilerParams(vmem_limit_bytes=12 * MIB),
        name="partial_sums",
    )(code, *sources, tiles)


def combine_kernel(near_ref, affinity_ref, parts_ref, out_ref, mixed_ref):
    classes, width = near_ref.shape
    power_at = classes - POWER_ROWS
    scales = []
    for p in range(PEERS):
        power = parts_ref[p, power_at:, :].astype(jnp.int32).astype(jnp.float32)[POWER_ROWS : POWER_ROWS + 1, :]
        scales.append(jnp.exp2(power - CODE_BITS))
    square = jnp.zeros((1, width), jnp.float32)
    for start in range(0, classes, CHUNK):
        at = slice(start, min(start + CHUNK, classes))
        total = near_ref[at, :]
        for p in range(PEERS):
            total += parts_ref[p, at, :].astype(jnp.int32).astype(jnp.float32) * scales[p]
        mixed = propagation_weight * total + affinity_ref[at, :].astype(jnp.float32)
        mixed_ref[at, :] = mixed
        square += jnp.sum(mixed * mixed, axis=0, keepdims=True)
    row_scale = lax.rsqrt(square * (1.0 / classes) + epsilon)
    for start in range(0, classes, CHUNK):
        at = slice(start, min(start + CHUNK, classes))
        out_ref[at, :] = (mixed_ref[at, :] * row_scale).astype(jnp.bfloat16)


def combine(near, affinity, parts):
    return pl.pallas_call(
        combine_kernel,
        out_shape=jax.ShapeDtypeStruct(near.shape, jnp.bfloat16),
        in_specs=[VMEM] * 3,
        out_specs=VMEM,
        scratch_shapes=[pltpu.VMEM(near.shape, jnp.float32)],
        cost_estimate=pl.CostEstimate(flops=1_000_000_000, bytes_accessed=3_000_000, transcendentals=0),
        compiler_params=pltpu.CompilerParams(vmem_limit_bytes=8 * MIB),
        name="combine",
    )(near, affinity, parts)


def local(inner, posterior, class_affinity, band_tiles, band_offset, band_count, far_tiles, far_row, far_block):
    size = band_tiles.shape[2]
    chips = SIDE * SIDE
    device = lax.axis_index("d")
    core, chip = (device % inner) % 2, device // inner
    order = jnp.asarray(tile_order())[core, chip]
    core = core.reshape(1)
    even = [(x * inner + j, x * inner + (j ^ 1)) for x in range(chips) for j in range(inner)]
    odd = [(x * inner + j, x * inner + (j + (1 if j % 2 else -1)) % inner) for x in range(chips) for j in range(inner)]

    def swap(value, phase, s):
        return lax.ppermute(value, "d", partner_pairs(inner, phase, s))

    current = posterior.T
    affinity = class_affinity.T
    for sweep in range(SWEEPS):
        sources = [current] + [None] * len(PARTNERS)
        for s in PARTNERS:
            sources[s] = swap(current, 0, s)
        if sweep == 0:
            payload = lax.all_to_all(
                pack(order, far_row.reshape(chips), far_block.reshape(chips), far_tiles.reshape(chips, size, size)),
                "d", 0, 0, tiled=True, axis_index_groups=square_groups(inner, 1),
            )
            code = payload[:, PEERS * size : PEERS * size + PEERS, 0].astype(jnp.int32)
        from_even = lax.ppermute(current, "d", even)
        from_odd = lax.ppermute(current, "d", odd)
        near = near_sum(core, band_offset, band_count, current, from_even, from_odd, band_tiles)
        part = partial_sums(code, sources, payload)
        parts = lax.all_to_all(part, "d", 0, 0, tiled=True, axis_index_groups=square_groups(inner, 1))
        current = combine(near, affinity, parts)
    return current.T


def solution(mesh):
    inner = mesh.shape["gy"]
    flat = Mesh(mesh.devices.reshape(-1), ("d",))
    spec = P("d")
    return jax.shard_map(
        lambda *args: local(inner, *args), mesh=flat, in_specs=(spec,) * 8, out_specs=spec, check_vma=False
    )
```
